8 devices in a mesh: row: 4 (over z, y, x), col: 2 (over core).
Axes of the slice: x: 2, y: 2, z: 1, core: 2. Of those that a mesh axis runs over, the one named last changes fastest.
Arguments:
- w_one: float32 [4, 2, 2, 768, 3072], P('row', 'col')
- w_two: float32 [4, 2, 2, 3072, 768], P('row', 'col')
- inputs: bfloat16 [4, 2, 3, 2048, 768], P('row', 'col')
- targets: bfloat16 [4, 2, 3, 2048, 768], P('row', 'col')
Outputs:
- output 1: float32 [4, 2, 2, 768, 3072], P('row', 'col')
- output 2: float32 [4, 2, 2, 3072, 768], P('row', 'col')
All inputs are finite; a program needn't handle non-finite values.
Results may differ from the reference program's by a relative error of at most 0.001.
Values are sent between devices in bfloat16 or wider.
A program may use at most 1 GiB of HBM per device.

```python
import jax
import jax.numpy as jnp
from jax import lax

GRID_ROWS = 4
GRID_COLS = 2
LAYERS = 2
NUM_STEPS = 3
BATCH_ROWS = 2048
D_MODEL = 768
D_FF = 3072

LEARN_RATE = 1.5
NORM_EPS = 1e-6
GELU_C = 0.7978845608028654
GELU_K = 0.044715
REPLICA_SPREAD = 0.5


def gelu_value(pre_act):
    tanh_inner = jnp.tanh(GELU_C * (pre_act + GELU_K * pre_act * pre_act * pre_act))
    return 0.5 * pre_act * (1.0 + tanh_inner)


def gelu_slope(pre_act):
    tanh_inner = jnp.tanh(GELU_C * (pre_act + GELU_K * pre_act * pre_act * pre_act))
    return 0.5 * (1.0 + tanh_inner) + 0.5 * pre_act * (1.0 - tanh_inner * tanh_inner) * GELU_C * (1.0 + 3.0 * GELU_K * pre_act * pre_act)


def setup_inputs(seed: int = 0) -> dict:
    root_key = jax.random.key(seed)
    sub_keys = jax.random.split(root_key, 6)
    grid_shape = (GRID_ROWS, GRID_COLS)
    shape_one = (LAYERS, D_MODEL, D_FF)
    shape_two = (LAYERS, D_FF, D_MODEL)
    norm_fac = (1.0 + REPLICA_SPREAD * REPLICA_SPREAD) ** -0.5
    base_one = jax.random.normal(sub_keys[0], shape_one, jnp.float32)
    own_one = jax.random.normal(sub_keys[1], grid_shape + shape_one, jnp.float32)
    w_one = (base_one + REPLICA_SPREAD * own_one) * (norm_fac * D_MODEL ** -0.5)
    base_two = jax.random.normal(sub_keys[2], shape_two, jnp.float32)
    own_two = jax.random.normal(sub_keys[3], grid_shape + shape_two, jnp.float32)
    w_two = (base_two + REPLICA_SPREAD * own_two) * (norm_fac * D_FF ** -0.5)
    data_shape = grid_shape + (NUM_STEPS, BATCH_ROWS, D_MODEL)
    inputs = jax.random.normal(sub_keys[4], data_shape, jnp.float32).astype(jnp.bfloat16)
    targets = jax.random.normal(sub_keys[5], data_shape, jnp.float32).astype(jnp.bfloat16)
    return {'w_one': w_one, 'w_two': w_two, 'inputs': inputs, 'targets': targets}


def local_update(w_one, w_two, x_in, target):
    one_lo = w_one.astype(jnp.bfloat16)
    two_lo = w_two.astype(jnp.bfloat16)
    hidden = x_in
    saved_acts = []
    for layer_idx in range(LAYERS):
        hid_f = hidden.astype(jnp.float32)
        inv_rms = lax.rsqrt(jnp.mean(hid_f * hid_f, axis=-1, keepdims=True) + NORM_EPS)
        normed = hid_f * inv_rms
        normed_lo = normed.astype(jnp.bfloat16)
        pre_act = jnp.dot(normed_lo, one_lo[layer_idx], preferred_element_type=jnp.float32)
        act_lo = gelu_value(pre_act).astype(jnp.bfloat16)
        mlp_out = jnp.dot(act_lo, two_lo[layer_idx], preferred_element_type=jnp.float32)
        saved_acts.append((normed, inv_rms, normed_lo, pre_act, act_lo))
        hidden = (hid_f + mlp_out).astype(jnp.bfloat16)
    d_hidden = (2.0 / (BATCH_ROWS * D_MODEL)) * (hidden.astype(jnp.float32) - target.astype(jnp.float32))
    grads_one = [None] * LAYERS
    grads_two = [None] * LAYERS
    for layer_idx in reversed(range(LAYERS)):
        normed, inv_rms, normed_lo, pre_act, act_lo = saved_acts[layer_idx]
        d_lo = d_hidden.astype(jnp.bfloat16)
        grads_two[layer_idx] = jnp.dot(act_lo.T, d_lo, preferred_element_type=jnp.float32)
        d_act = jnp.dot(d_lo, two_lo[layer_idx].T, preferred_element_type=jnp.float32)
        d_pre = (d_act * gelu_slope(pre_act)).astype(jnp.bfloat16)
        grads_one[layer_idx] = jnp.dot(normed_lo.T, d_pre, preferred_element_type=jnp.float32)
        if layer_idx > 0:
            d_normed = jnp.dot(d_pre, one_lo[layer_idx].T, preferred_element_type=jnp.float32)
            d_hidden = d_hidden + inv_rms * (d_normed - normed * jnp.mean(d_normed * normed, axis=-1, keepdims=True))
    return w_one - LEARN_RATE * jnp.stack(grads_one), w_two - LEARN_RATE * jnp.stack(grads_two)


def gossip_mix(upd_vals):
    wire_vals = upd_vals.astype(jnp.bfloat16)
    mix_sum = upd_vals + jnp.roll(wire_vals, 1, axis=1).astype(jnp.float32)
    mix_sum = mix_sum + jnp.roll(wire_vals, -1, axis=1).astype(jnp.float32)
    mix_sum = mix_sum + jnp.roll(wire_vals, 1, axis=0).astype(jnp.float32)
    mix_sum = mix_sum + jnp.roll(wire_vals, -1, axis=0).astype(jnp.float32)
    return mix_sum / 5.0


def reference(w_one, w_two, inputs, targets):
    n_rep = GRID_ROWS * GRID_COLS
    for step_idx in range(NUM_STEPS):
        flat_one = w_one.reshape((n_rep, LAYERS, D_MODEL, D_FF))
        flat_two = w_two.reshape((n_rep, LAYERS, D_FF, D_MODEL))
        x_step = inputs[:, :, step_idx].reshape((n_rep, BATCH_ROWS, D_MODEL))
        t_step = targets[:, :, step_idx].reshape((n_rep, BATCH_ROWS, D_MODEL))
        upd_one, upd_two = lax.map(lambda packed: local_update(packed[0], packed[1], packed[2], packed[3]), (flat_one, flat_two, x_step, t_step))
        w_one = gossip_mix(upd_one.reshape(w_one.shape))
        w_two = gossip_mix(upd_two.reshape(w_two.shape))
    return w_one, w_two
```

```python
import jax
import jax.numpy as jnp
from jax import lax
from jax.experimental import pallas as pl
from jax.experimental.pallas import tpu as pltpu
from jax.sharding import PartitionSpec as P


LEARN_RATE = 1.5
NORM_EPS = 1e-6
GELU_C = 0.7978845608028654
GELU_K = 0.044715

BF = jnp.bfloat16
F32 = jnp.float32
VMEM_LIMIT = 60 * 1024 * 1024
ROWS = 256
KROWS = 512
SUB = 256


ANY = pl.BlockSpec(memory_space=pl.ANY)


def nn(lhs, rhs):
    return lax.dot_general(lhs, rhs, (((1,), (0,)), ((), ())), preferred_element_type=F32)


def nt(lhs, rhs):
    return lax.dot_general(lhs, rhs, (((1,), (1,)), ((), ())), preferred_element_type=F32)


def view(arr, lead, shape, row_blk=0, col_blk=0):
    return (arr, lead, shape, row_blk, col_blk)


def whole(v):
    _, lead, shape, rb, cb = v
    return pl.BlockSpec((None,) * len(lead) + shape, lambda i: lead + (rb, cb))


def by_rows(v, rows):
    _, lead, shape, rb, cb = v
    steps = shape[0] // rows
    return pl.BlockSpec((None,) * len(lead) + (rows, shape[1]), lambda i: lead + (rb * steps + i, cb))


def run(kernel, grid, ins, outs, aliases=None, scratch=(), flops=0, nbytes=0):
    return pl.pallas_call(
        kernel,
        grid=(grid,),
        in_specs=[spec for _, spec in ins],
        out_specs=[spec for _, spec in outs],
        out_shape=[shape for shape, _ in outs],
        input_output_aliases=aliases or {},
        scratch_shapes=list(scratch),
        compiler_params=pltpu.CompilerParams(dimension_semantics=("arbitrary",), vmem_limit_bytes=VMEM_LIMIT),
        cost_estimate=pl.CostEstimate(flops=int(flops), bytes_accessed=int(nbytes), transcendentals=0),
    )(*[v[0] if isinstance(v, tuple) else v for v, _ in ins])


def norm_of(h):
    x = h.astype(F32)
    inv = lax.rsqrt(jnp.mean(x * x, axis=-1, keepdims=True) + NORM_EPS)
    return x * inv, inv


def fwd_one(h, units, prev, off):
    rows, d = h[2]
    width = units[0][2][1]
    f = 4 * width
    nu = len(units)

    def kernel(h_ref, *refs):
        w_refs, (a_ref, s_ref) = refs[:nu], refs[-2:]
        n, _ = norm_of(h_ref[...])
        n = n.astype(BF)
        for j in range(nu):
            for c in range(0, width, SUB):
                z = nn(n, w_refs[j][:, c:c + SUB].astype(BF))
                t = jnp.tanh(GELU_C * (z + GELU_K * z * z * z))
                cols = slice(j * width + c, j * width + c + SUB)
                a_ref[:, cols] = (0.5 * z * (1.0 + t)).astype(BF)
                s_ref[:, cols] = 0.5 * (1.0 + t) + 0.5 * z * (1.0 - t * t) * GELU_C * (1.0 + 3.0 * GELU_K * z * z)

    blk = pl.BlockSpec((ROWS, nu * width), lambda i: (i, off // nu))
    ins = [(h, by_rows(h, ROWS))] + [(u, whole(u)) for u in units]
    aliases = None
    if prev is not None:
        aliases = {len(ins): 0, len(ins) + 1: 1}
        ins += [(p, ANY) for p in prev]
    return run(kernel, rows // ROWS, ins, [(jax.ShapeDtypeStruct((rows, f), BF), blk), (jax.ShapeDtypeStruct((rows, f), F32), blk)],
               aliases, flops=2 * rows * d * width * nu, nbytes=6 * rows * width * nu)


def fwd_two(h, a, units):
    rows, d = h[2]
    nu = len(units)
    f = a.shape[1]
    part = f // nu
    av = view(a, (), (rows, f))

    def kernel(h_ref, a_ref, *refs):
        w_refs, o_ref = refs[:nu], refs[nu]
        for c in range(0, d, SUB):
            acc = nn(a_ref[:, :part], w_refs[0][:, c:c + SUB].astype(BF))
            for j in range(1, nu):
                acc += nn(a_ref[:, j * part:(j + 1) * part], w_refs[j][:, c:c + SUB].astype(BF))
            o_ref[:, c:c + SUB] = (h_ref[:, c:c + SUB].astype(F32) + acc).astype(BF)

    ov = view(None, (), (rows, d))
    return run(kernel, rows // ROWS, [(h, by_rows(h, ROWS)), (av, by_rows(av, ROWS))] + [(u, whole(u)) for u in units],
               [(jax.ShapeDtypeStruct((rows, d), BF), by_rows(ov, ROWS))], flops=2 * rows * d * f, nbytes=2 * rows * f)[0]


def fwd_loss(h, a, unit, target, idx, d):
    rows, f = a.shape
    w = unit[2][1]
    scale = 2.0 / (rows * d)
    hv = view(h, (), (rows, w), 0, idx)
    tv = (target[0], target[1], (rows, w), 0, idx)
    av = view(a, (), (rows, f))

    def kernel(h_ref, t_ref, a_ref, w_ref, e_ref, b_ref):
        out = (h_ref[...].astype(F32) + nn(a_ref[...], w_ref[...].astype(BF))).astype(BF)
        e = scale * (out.astype(F32) - t_ref[...].astype(F32))
        e_ref[...] = e
        b_ref[...] = e.astype(BF)

    ov = view(None, (), (rows, w))
    return run(kernel, rows // ROWS, [(hv, by_rows(hv, ROWS)), (tv, by_rows(tv, ROWS)), (av, by_rows(av, ROWS)), (unit, whole(unit))],
               [(jax.ShapeDtypeStruct((rows, w), F32), by_rows(ov, ROWS)), (jax.ShapeDtypeStruct((rows, w), BF), by_rows(ov, ROWS))],
               flops=2 * rows * w * f, nbytes=2 * rows * f)


def back_act(errs, units, slope):
    rows, f = slope.shape
    ne, nu = len(errs), len(units)
    per = units[0][2][0]

    def kernel(*refs):
        e_refs, w_refs = refs[:ne], refs[ne:ne + nu]
        s_ref, o_ref = refs[ne + nu:]
        for c in range(0, f, SUB):
            if ne > 1:
                u = nt(e_refs[0][...], w_refs[0][c:c + SUB, :].astype(BF))
                for k in range(1, ne):
                    u += nt(e_refs[k][...], w_refs[k][c:c + SUB, :].astype(BF))
            else:
                r = c % per
                u = nt(e_refs[0][...], w_refs[c // per][r:r + SUB, :].astype(BF))
            o_ref[:, c:c + SUB] = (u * s_ref[:, c:c + SUB]).astype(BF)

    vs = [view(e, (), e.shape) for e in errs]
    sv = view(slope, (), (rows, f))
    return run(kernel, rows // ROWS, [(v, by_rows(v, ROWS)) for v in vs] + [(u, whole(u)) for u in units] + [(sv, by_rows(sv, ROWS))],
               [(jax.ShapeDtypeStruct((rows, f), BF), by_rows(sv, ROWS))], flops=2 * rows * f * 768, nbytes=6 * rows * f)[0]


def back_norm(dz, units, h, errs):
    rows, f = dz.shape
    d = h[2][1]
    ne, nu = len(errs), len(units)
    per = f // nu

    def kernel(dz_ref, *refs):
        w_refs, h_ref, e_refs, o_ref, m_ref = refs[:nu], refs[nu], refs[nu + 1:nu + 1 + ne], refs[-2], refs[-1]
        for c in range(0, d, SUB):
            m = nt(dz_ref[:, :per], w_refs[0][c:c + SUB, :].astype(BF))
            for j in range(1, nu):
                m += nt(dz_ref[:, j * per:(j + 1) * per], w_refs[j][c:c + SUB, :].astype(BF))
            m_ref[:, c:c + SUB] = m
        n, inv = norm_of(h_ref[...])
        m = m_ref[...]
        back = inv * (m - n * jnp.mean(m * n, axis=-1, keepdims=True))
        w = d // ne
        for k in range(ne):
            o_ref[:, k * w:(k + 1) * w] = (e_refs[k][...] + back[:, k * w:(k + 1) * w]).astype(BF)

    dv = view(dz, (), (rows, f))
    vs = [view(e, (), e.shape) for e in errs]
    ov = view(None, (), (rows, d))
    return run(kernel, rows // ROWS,
               [(dv, by_rows(dv, ROWS))] + [(u, whole(u)) for u in units] + [(h, by_rows(h, ROWS))] + [(v, by_rows(v, ROWS)) for v in vs],
               [(jax.ShapeDtypeStruct((rows, d), BF), by_rows(ov, ROWS))], scratch=[pltpu.VMEM((ROWS, d), F32)],
               flops=2 * rows * f * d, nbytes=2 * rows * f)[0]


def grad_update(small, big, olds, use_norm, flip):
    rows, m = small[2]
    n = big[2][1]
    nu = len(olds)
    per = n // nu
    steps = rows // KROWS

    def kernel(s_ref, b_ref, *refs):
        p_refs, q_refs, w_refs, acc_ref = refs[:nu], refs[nu:2 * nu], refs[2 * nu:3 * nu], refs[-1]
        i = pl.program_id(0)
        s = s_ref[...]
        if use_norm:
            s = norm_of(s)[0].astype(BF)
        st = s.T

        @pl.when(i == 0)
        def _():
            for c in range(0, n, SUB):
                acc_ref[:, c:c + SUB] = nn(st, b_ref[:, c:c + SUB])

        @pl.when(i > 0)
        def _():
            for c in range(0, n, SUB):
                acc_ref[:, c:c + SUB] += nn(st, b_ref[:, c:c + SUB])

        @pl.when(i == steps - 1)
        def _():
            for j in range(nu):
                for c in range(0, per, SUB):
                    g = acc_ref[:, j * per + c:j * per + c + SUB]
                    at = (slice(c, c + SUB), slice(None)) if flip else (slice(None), slice(c, c + SUB))
                    q = p_refs[j][at] - LEARN_RATE * (g.T if flip else g)
                    q_refs[j][at] = q
                    w_refs[j][at] = q.astype(BF)

    def out(u, dt):
        shape = u[2]
        return (jax.ShapeDtypeStruct(shape, dt), pl.BlockSpec(shape, lambda i: (0, 0)))

    res = run(kernel, steps, [(small, by_rows(small, KROWS)), (big, by_rows(big, KROWS))] + [(u, whole(u)) for u in olds],
              [out(u, F32) for u in olds] + [out(u, BF) for u in olds], scratch=[pltpu.VMEM((m, n), F32)],
              flops=2 * rows * m * n, nbytes=10 * m * n)
    return res[:nu], res[nu:]


def combine(even, own, cc, xx, yy, final):
    rows, cols = own.shape
    blk = 256 if cols > 512 else 768

    def kernel(even_ref, q_ref, c_ref, x_ref, y_ref, *refs):
        prev = jnp.where(even_ref[0] == 1, y_ref[...], x_ref[...]).astype(F32)
        nxt = jnp.where(even_ref[0] == 1, x_ref[...], y_ref[...]).astype(F32)
        c = c_ref[...].astype(F32)
        p = (q_ref[...] + c + c + prev + nxt) / 5.0
        if final is None:
            refs[0][...] = p
            refs[1][...] = p.astype(BF)
        else:
            refs[-1][...] = p

    ov = view(None, (), (rows, cols))
    spec = by_rows(ov, blk)
    ins = [(even, pl.BlockSpec(memory_space=pltpu.SMEM))] + [(v, spec) for v in (own, cc, xx, yy)]
    if final is None:
        return run(kernel, rows // blk, ins, [(jax.ShapeDtypeStruct((rows, cols), F32), spec), (jax.ShapeDtypeStruct((rows, cols), BF), spec)],
                   nbytes=18 * rows * cols, flops=8 * rows * cols)
    arr, shape, layer, rb, cb = final
    aliases = None
    if arr is not None:
        aliases = {len(ins): 0}
        ins.append((arr, ANY))
    fv = (None, (0, 0, layer), (rows, cols), rb, cb)
    return run(kernel, rows // blk, ins, [(jax.ShapeDtypeStruct(shape, F32), by_rows(fv, blk))], aliases, nbytes=14 * rows * cols, flops=8 * rows * cols)


X_SWAP = [(0, 1), (1, 0), (2, 3), (3, 2)]
Y_SWAP = [(0, 2), (2, 0), (1, 3), (3, 1)]
C_SWAP = [(0, 1), (1, 0)]

L1B = ["A", "B", "C"]
ONE0 = ["a0", "a1", "a2", "a3"]
TWO0 = ["b0", "b1", "b2", "b3"]
ONE1 = ["d0", "d1", "d2", "d3"]
WIRE = ["A", "B"] + ONE0 + TWO0 + ONE1 + ["C"]
N_STEPS = 3


def graph():
    ops = {}

    def comp(name, us, needs, pri):
        ops[name] = ("tc", us, list(needs), pri)

    for t in range(N_STEPS):
        def w(units):
            return [f"comb{t - 1}_{u}" for u in units] if t else []

        base = t * 1000
        comp(f"f1a{t}_0", 8, w(ONE0[:2]), base + 10)
        comp(f"f1b{t}_0", 8, w(ONE0[2:]) + [f"f1a{t}_0"], base + 11)
        comp(f"f2{t}_0", 13, w(TWO0) + [f"f1b{t}_0"], base + 12)
        comp(f"f1a{t}_1", 8, w(ONE1[:2]) + [f"f2{t}_0"], base + 13)
        comp(f"f1b{t}_1", 8, w(ONE1[2:]) + [f"f1a{t}_1"], base + 14)
        for k, u in enumerate(L1B):
            comp(f"fl{t}_{u}", 6, w([u]) + [f"f1b{t}_1"], base + 20 + (0 if u == "A" else 10 + k))
            comp(f"g2{t}_{u}", 7, [f"fl{t}_{u}"], base + 21 + (0 if u == "A" else 14 + k if u == "B" else 500))
        comp(f"u{t}_1", 13, [f"fl{t}_{u}" for u in L1B] + w(L1B), base + 40)
        comp(f"m{t}", 13, [f"u{t}_1"] + w(ONE1), base + 41)
        comp(f"u{t}_0", 13, [f"m{t}"] + w(TWO0), base + 42)
        for h in (0, 1):
            comp(f"g1{t}_0{h}", 9, [f"u{t}_0"] + w(ONE0[2 * h:2 * h + 2]), base + 50 + h)
            comp(f"g2{t}_0{h}", 9, [f"m{t}"] + w(TWO0[2 * h:2 * h + 2]), base + 60 + h)
            comp(f"g1{t}_1{h}", 9, [f"u{t}_1"] + w(ONE1[2 * h:2 * h + 2]), base + 70 + h)
        made = {u: f"g2{t}_{u}" for u in L1B}
        for h in (0, 1):
            for j in (2 * h, 2 * h + 1):
                made[ONE0[j]], made[TWO0[j]], made[ONE1[j]] = f"g1{t}_0{h}", f"g2{t}_0{h}", f"g1{t}_1{h}"
        for k, u in enumerate(WIRE):
            us = 35.5 if u in L1B else 26.6
            ops[f"x{t}_{u}"] = ("x", us, [made[u]], k)
            ops[f"y{t}_{u}"] = ("y", us, [f"x{t}_{u}"], k)
            ops[f"c{t}_{u}"] = ("c", 3, [made[u]], k)
            comp(f"comb{t}_{u}", 5 if u in L1B else 4, [f"{r}{t}_{u}" for r in "xyc"] + [made[u]], base + 5)
    return ops


DEPTH = 2
MARGIN = 1.5


def plan():
    ops = graph()
    queue = {r: [f"{r}{t}_{u}" for t in range(N_STEPS) for u in WIRE] for r in "xyc"}
    end = {}
    link_end = {r: [] for r in "xyc"}
    order = []
    todo = [n for n in ops if ops[n][0] == "tc"]
    now = 0.0
    while todo or any(queue.values()):
        moved = True
        while moved:
            moved = False
            for r in "ycx":
                while queue[r]:
                    n = queue[r][0]
                    needs = ops[n][2]
                    if not all(d in end and end[d] + (MARGIN if r == "y" else 0) <= now for d in needs):
                        break
                    live = [e for e in link_end[r] if e > now]
                    if len(live) >= DEPTH and r != "c" and False:
                        break
                    begin = max(now, link_end[r][-1] if link_end[r] else 0.0) + 1.0
                    link_end[r].append(begin + ops[n][1])
                    end[n] = link_end[r][-1]
                    order.append(n)
                    queue[r].pop(0)
                    now += 0.7
                    moved = True
        ready = [n for n in todo if all(d in end and end[d] + (MARGIN if d[0] in "xyc" and not d.startswith("comb") else 0) <= now for d in ops[n][2])]
        if ready:
            n = min(ready, key=lambda m: ops[m][3])
            todo.remove(n)
            now += ops[n][1]
            end[n] = now
            order.append(n)
        else:
            later = [e + MARGIN for e in end.values() if e + MARGIN > now + 1e-9]
            now = min(later)
    return order, max(end.values()), end


def solution(mesh):
    def device_fn(w_one, w_two, inputs, targets):
        _, d, f = w_one.shape[2:]
        rows = inputs.shape[3]
        quarter = f // 4
        third = d // 3
        even = (1 - lax.rem(lax.axis_index("row"), 2)).astype(jnp.int32).reshape((1,))
        master, low = {}, {}
        for j in range(4):
            for lay, names in ((0, ONE0), (1, ONE1)):
                master[names[j]] = view(w_one, (0, 0, lay), (d, quarter), 0, j)
            master[TWO0[j]] = view(w_two, (0, 0, 0), (quarter, d), j, 0)
        for j, u in enumerate(L1B):
            master[u] = view(w_two, (0, 0, 1), (f, third), 0, j)
        low.update(master)
        where = {}
        for j in range(4):
            where[ONE0[j]], where[ONE1[j]], where[TWO0[j]] = ("one", 0, 0, j), ("one", 1, 0, j), ("two", 0, j, 0)
        for j, u in enumerate(L1B):
            where[u] = ("two", 1, 0, j)
        final = {"one": None, "two": None}
        shapes = {"one": w_one.shape, "two": w_two.shape}
        st = {}
        own, wire, moved = {}, {}, {}

        def issue(name):
            if name[0] in "xyc" and not name.startswith("comb"):
                r, t, u = name[0], int(name[1]), name.split("_")[1]
                if r == "x":
                    moved[name] = lax.ppermute(wire[t, u], "row", X_SWAP)
                elif r == "y":
                    moved[name] = lax.ppermute(moved[f"x{t}_{u}"], "row", Y_SWAP)
                else:
                    moved[name] = lax.ppermute(wire[t, u], "col", C_SWAP)
                return
            kind, rest = name.split("_")
            t = int(kind[-1])
            kind = kind[:-1]
            x_in = view(inputs, (0, 0, t), (rows, d))
            target = view(targets, (0, 0, t), (rows, d))
            if kind == "comb":
                u = rest
                args = (even, own[t, u], moved[f"c{t}_{u}"], moved[f"x{t}_{u}"], moved[f"y{t}_{u}"])
                if t == N_STEPS - 1:
                    which, layer, rb, cb = where[u]
                    final[which] = combine(*args, (final[which], shapes[which], layer, rb, cb))[0]
                else:
                    p, b = combine(*args, None)
                    master[u], low[u] = view(p, (), p.shape), view(b, (), b.shape)
            elif kind in ("f1a", "f1b"):
                lay = int(rest)
                names = (ONE0, ONE1)[lay]
                h = x_in if lay == 0 else view(st["h", t], (), (rows, d))
                first = kind == "f1a"
                us = names[:2] if first else names[2:]
                prev = None if first else (st["a", t, lay], st["s", t, lay])
                st["a", t, lay], st["s", t, lay] = fwd_one(h, [low[u] for u in us], prev, 0 if first else 2)
            elif kind == "f2":
                st["h", t] = fwd_two(x_in, st["a", t, 0], [low[u] for u in TWO0])
            elif kind == "fl":
                st["e", t, rest], st["eb", t, rest] = fwd_loss(st["h", t], st["a", t, 1], low[rest], target, L1B.index(rest), d)
            elif kind == "u" and rest == "1":
                st["dz", t, 1] = back_act([st["eb", t, u] for u in L1B], [low[u] for u in L1B], st["s", t, 1])
            elif kind == "u":
                st["dz", t, 0] = back_act([st["e0", t]], [low[u] for u in TWO0], st["s", t, 0])
            elif kind == "g2" and rest in L1B:
                eb = st["eb", t, rest]
                a = st["a", t, 1]
                q, b = grad_update(view(eb, (), eb.shape), view(a, (), a.shape), [master[rest]], False, True)
                own[t, rest], wire[t, rest] = q[0], b[0]
            elif kind in ("g1", "g2"):
                lay, half = int(rest[0]), int(rest[1])
                if kind == "g1":
                    names = (ONE0, ONE1)[lay]
                    small = x_in if lay == 0 else view(st["h", t], (), (rows, d))
                    big = view(st["dz", t, lay], (), (rows, f // 2), 0, half)
                else:
                    names = TWO0
                    small = view(st["e0", t], (), (rows, d))
                    big = view(st["a", t, 0], (), (rows, f // 2), 0, half)
                us = names[2 * half:2 * half + 2]
                q, b = grad_update(small, big, [master[u] for u in us], kind == "g1", kind == "g2")
                for k, u in enumerate(us):
                    own[t, u], wire[t, u] = q[k], b[k]

        order = plan()[0]
        for name in order:
            if name.startswith("m") :
                t = int(name[1])
                st["e0", t] = back_norm(st["dz", t, 1], [low[u] for u in ONE1], view(st["h", t], (), (rows, d)), [st["e", t, u] for u in L1B])
            else:
                issue(name)
        return final["one"], final["two"]

    spec = P("row", "col")
    return jax.shard_map(device_fn, mesh=mesh, in_specs=(spec,) * 4, out_specs=(spec, spec), check_vma=False)
```

```python
import jax
import jax.numpy as jnp
from jax import lax
from jax.experimental import pallas as pl
from jax.experimental.pallas import tpu as pltpu
from jax.sharding import PartitionSpec as P


LEARN_RATE = 1.5
NORM_EPS = 1e-6
GELU_C = 0.7978845608028654
GELU_K = 0.044715

BF = jnp.bfloat16
F32 = jnp.float32
VMEM_LIMIT = 60 * 1024 * 1024
ROWS = 256
MROWS = 512
LROWS = 1024
KROWS = 512
SUB = 256


ANY = pl.BlockSpec(memory_space=pl.ANY)


def nn(lhs, rhs):
    return lax.dot_general(lhs, rhs, (((1,), (0,)), ((), ())), preferred_element_type=F32)


def nt(lhs, rhs):
    return lax.dot_general(lhs, rhs, (((1,), (1,)), ((), ())), preferred_element_type=F32)


def view(arr, lead, shape, row_blk=0, col_blk=0):
    return (arr, lead, shape, row_blk, col_blk)


def whole(v):
    _, lead, shape, rb, cb = v
    return pl.BlockSpec((None,) * len(lead) + shape, lambda i: lead + (rb, cb))


def by_rows(v, rows):
    _, lead, shape, rb, cb = v
    steps = shape[0] // rows
    return pl.BlockSpec((None,) * len(lead) + (rows, shape[1]), lambda i: lead + (rb * steps + i, cb))


def run(kernel, grid, ins, outs, aliases=None, scratch=(), flops=0, nbytes=0):
    return pl.pallas_call(
        kernel,
        grid=(grid,),
        in_specs=[spec for _, spec in ins],
        out_specs=[spec for _, spec in outs],
        out_shape=[shape for shape, _ in outs],
        input_output_aliases=aliases or {},
        scratch_shapes=list(scratch),
        compiler_params=pltpu.CompilerParams(dimension_semantics=("arbitrary",), vmem_limit_bytes=VMEM_LIMIT),
        cost_estimate=pl.CostEstimate(flops=int(flops), bytes_accessed=int(nbytes), transcendentals=0),
    )(*[v[0] if isinstance(v, tuple) else v for v, _ in ins])


def norm_of(h):
    x = h.astype(F32)
    inv = lax.rsqrt(jnp.mean(x * x, axis=-1, keepdims=True) + NORM_EPS)
    return x * inv, inv


def fwd_one(h, units, prev, off):
    rows, d = h[2]
    width = units[0][2][1]
    f = 4 * width
    nu = len(units)
    rb = ROWS if nu > 1 else 2 * ROWS

    def kernel(h_ref, *refs):
        w_refs, (a_ref, s_ref) = refs[:nu], refs[-2:]
        n, _ = norm_of(h_ref[...])
        n = n.astype(BF)
        for j in range(nu):
            for c in range(0, width, SUB):
                z = nn(n, w_refs[j][:, c:c + SUB].astype(BF))
                z2 = z * z
                t = jnp.tanh(z * (GELU_C + (GELU_C * GELU_K) * z2))
                half = 0.5 + 0.5 * t
                a = z * half
                cols = slice(j * width + c, j * width + c + SUB)
                a_ref[:, cols] = a.astype(BF)
                s_ref[:, cols] = half + a * (1.0 - t) * (GELU_C + (3.0 * GELU_C * GELU_K) * z2)

    blk = pl.BlockSpec((rb, nu * width), lambda i: (i, off // nu))
    ins = [(h, by_rows(h, rb))] + [(u, whole(u)) for u in units]
    aliases = None
    if prev is not None:
        aliases = {len(ins): 0, len(ins) + 1: 1}
        ins += [(p, ANY) for p in prev]
    return run(kernel, rows // rb, ins, [(jax.ShapeDtypeStruct((rows, f), BF), blk), (jax.ShapeDtypeStruct((rows, f), F32), blk)],
               aliases, flops=2 * rows * d * width * nu, nbytes=6 * rows * width * nu)


def fwd_two(h, a, units):
    rows, d = h[2]
    nu = len(units)
    f = a.shape[1]
    part = f // nu
    av = view(a, (), (rows, f))

    def kernel(h_ref, a_ref, *refs):
        w_refs, o_ref = refs[:nu], refs[nu]
        for c in range(0, d, SUB):
            acc = nn(a_ref[:, :part], w_refs[0][:, c:c + SUB].astype(BF))
            for j in range(1, nu):
                acc += nn(a_ref[:, j * part:(j + 1) * part], w_refs[j][:, c:c + SUB].astype(BF))
            o_ref[:, c:c + SUB] = (h_ref[:, c:c + SUB].astype(F32) + acc).astype(BF)

    ov = view(None, (), (rows, d))
    return run(kernel, rows // MROWS, [(h, by_rows(h, MROWS)), (av, by_rows(av, MROWS))] + [(u, whole(u)) for u in units],
               [(jax.ShapeDtypeStruct((rows, d), BF), by_rows(ov, MROWS))], flops=2 * rows * d * f, nbytes=2 * rows * f)[0]


def fwd_loss(h, a, unit, target, idx, d):
    rows, f = a.shape
    w = unit[2][1]
    scale = 2.0 / (rows * d)
    hv = view(h, (), (rows, w), 0, idx)
    tv = (target[0], target[1], (rows, w), 0, idx)
    av = view(a, (), (rows, f))

    def kernel(h_ref, t_ref, a_ref, w_ref, e_ref, b_ref):
        out = (h_ref[...].astype(F32) + nn(a_ref[...], w_ref[...].astype(BF))).astype(BF)
        e = scale * (out.astype(F32) - t_ref[...].astype(F32))
        e_ref[...] = e
        b_ref[...] = e.astype(BF)

    ov = view(None, (), (rows, w))
    return run(kernel, rows // LROWS, [(hv, by_rows(hv, LROWS)), (tv, by_rows(tv, LROWS)), (av, by_rows(av, LROWS)), (unit, whole(unit))],
               [(jax.ShapeDtypeStruct((rows, w), F32), by_rows(ov, LROWS)), (jax.ShapeDtypeStruct((rows, w), BF), by_rows(ov, LROWS))],
               flops=2 * rows * w * f, nbytes=2 * rows * f)


def back_act(errs, units, slope, lo=0, of=1):
    rows, f = slope.shape
    f = f // of
    ne, nu = len(errs), len(units)
    per = units[0][2][0]

    def kernel(*refs):
        e_refs, w_refs = refs[:ne], refs[ne:ne + nu]
        s_ref, o_ref = refs[ne + nu:]
        for c in range(0, f, SUB):
            if ne > 1:
                u = nt(e_refs[0][...], w_refs[0][c:c + SUB, :].astype(BF))
                for k in range(1, ne):
                    u += nt(e_refs[k][...], w_refs[k][c:c + SUB, :].astype(BF))
            else:
                r = c % per
                u = nt(e_refs[0][...], w_refs[c // per][r:r + SUB, :].astype(BF))
            o_ref[:, c:c + SUB] = (u * s_ref[:, c:c + SUB]).astype(BF)

    vs = [view(e, (), e.shape) for e in errs]
    sv = view(slope, (), (rows, f), 0, lo)
    ov = view(None, (), (rows, f))
    return run(kernel, rows // MROWS, [(v, by_rows(v, MROWS)) for v in vs] + [(u, whole(u)) for u in units] + [(sv, by_rows(sv, MROWS))],
               [(jax.ShapeDtypeStruct((rows, f), BF), by_rows(ov, MROWS))], flops=2 * rows * f * 768, nbytes=6 * rows * f)[0]


def back_norm(dz, units, h, errs):
    rows, f = dz.shape
    d = h[2][1]
    ne, nu = len(errs), len(units)
    per = f // nu

    def kernel(dz_ref, *refs):
        w_refs, h_ref, e_refs, o_ref, m_ref = refs[:nu], refs[nu], refs[nu + 1:nu + 1 + ne], refs[-2], refs[-1]
        for c in range(0, d, SUB):
            m = nt(dz_ref[:, :per], w_refs[0][c:c + SUB, :].astype(BF))
            for j in range(1, nu):
                m += nt(dz_ref[:, j * per:(j + 1) * per], w_refs[j][c:c + SUB, :].astype(BF))
            m_ref[:, c:c + SUB] = m
        n, inv = norm_of(h_ref[...])
        m = m_ref[...]
        back = inv * (m - n * jnp.mean(m * n, axis=-1, keepdims=True))
        w = d // ne
        for k in range(ne):
            o_ref[:, k * w:(k + 1) * w] = (e_refs[k][...] + back[:, k * w:(k + 1) * w]).astype(BF)

    dv = view(dz, (), (rows, f))
    vs = [view(e, (), e.shape) for e in errs]
    ov = view(None, (), (rows, d))
    return run(kernel, rows // MROWS,
               [(dv, by_rows(dv, MROWS))] + [(u, whole(u)) for u in units] + [(h, by_rows(h, MROWS))] + [(v, by_rows(v, MROWS)) for v in vs],
               [(jax.ShapeDtypeStruct((rows, d), BF), by_rows(ov, MROWS))], scratch=[pltpu.VMEM((MROWS, d), F32)],
               flops=2 * rows * f * d, nbytes=2 * rows * f)[0]


def grad_update(small, big, olds, cuts, use_norm, flip):
    rows, m = small[2]
    n = big[2][1]
    nu = len(olds)
    per = n // nu
    steps = rows // KROWS
    out_shapes, out_kinds = [], []
    for j, u in enumerate(olds):
        r, c = u[2]
        out_shapes += [((r, c), F32), ((r, c), BF)] + ([((r // cuts[j], c), BF)] * cuts[j] if cuts[j] > 1 else [])
        out_kinds += [(j, -2), (j, -1)] + ([(j, k) for k in range(cuts[j])] if cuts[j] > 1 else [])

    def kernel(s_ref, b_ref, *refs):
        p_refs, o_refs, acc_ref = refs[:nu], refs[nu:-1], refs[-1]
        i = pl.program_id(0)
        s = s_ref[...]
        if use_norm:
            s = norm_of(s)[0].astype(BF)
        st = s.T

        @pl.when(i == 0)
        def _():
            for c in range(0, n, SUB):
                acc_ref[:, c:c + SUB] = nn(st, b_ref[:, c:c + SUB])

        @pl.when(i > 0)
        def _():
            for c in range(0, n, SUB):
                acc_ref[:, c:c + SUB] += nn(st, b_ref[:, c:c + SUB])

        @pl.when(i == steps - 1)
        def _():
            for (j, kind), o_ref in zip(out_kinds, o_refs):
                if kind != -2:
                    continue
                w_ref = o_refs[out_kinds.index((j, -1))]
                pieces = [o_refs[out_kinds.index((j, k))] for k in range(cuts[j])] if cuts[j] > 1 else []
                size = olds[j][2][0] // cuts[j]
                for c in range(0, per, SUB):
                    g = acc_ref[:, j * per + c:j * per + c + SUB]
                    at = (slice(c, c + SUB), slice(None)) if flip else (slice(None), slice(c, c + SUB))
                    q = p_refs[j][at] - LEARN_RATE * (g.T if flip else g)
                    low = q.astype(BF)
                    o_ref[at] = q
                    w_ref[at] = low
                    for k, piece in enumerate(pieces):
                        if flip:
                            if c // size == k:
                                piece[c - k * size:c - k * size + SUB, :] = low
                        else:
                            piece[:, c:c + SUB] = low[k * size:(k + 1) * size]

    res = run(kernel, steps, [(small, by_rows(small, KROWS)), (big, by_rows(big, KROWS))] + [(u, whole(u)) for u in olds],
              [(jax.ShapeDtypeStruct(sh, dt), pl.BlockSpec(sh, lambda i: (0, 0))) for sh, dt in out_shapes],
              scratch=[pltpu.VMEM((m, n), F32)], flops=2 * rows * m * n, nbytes=10 * m * n)
    got = {kind: r for kind, r in zip(out_kinds, res)}
    return [(got[j, -2], got[j, -1], [got[j, k] for k in range(cuts[j])] if cuts[j] > 1 else [got[j, -1]]) for j in range(nu)]


COMB_ROWS = {768: 256, 256: 768}


def combine(even, own, cc, xx, yy, final):
    rows, cols = own.shape
    nc = len(xx)
    blk = rows // nc if nc > 1 else COMB_ROWS[cols]

    def kernel(even_ref, q_ref, c_ref, *refs):
        def mix(x, y):
            prev = jnp.where(even_ref[0] == 1, y, x).astype(F32)
            nxt = jnp.where(even_ref[0] == 1, x, y).astype(F32)
            c = c_ref[...].astype(F32)
            p = (q_ref[...] + c + c + prev + nxt) / 5.0
            if final is None:
                refs[2 * nc][...] = p
                refs[2 * nc + 1][...] = p.astype(BF)
            else:
                refs[-1][...] = p

        if nc == 1:
            mix(refs[0][...], refs[1][...])
        else:
            for k in range(nc):
                @pl.when(pl.program_id(0) == k)
                def _(k=k):
                    mix(refs[k][...], refs[nc + k][...])

    ov = view(None, (), (rows, cols))
    spec = by_rows(ov, blk)
    pv = view(None, (), (rows // nc, cols))
    piece = by_rows(pv, blk) if nc == 1 else whole(pv)
    ins = [(even, pl.BlockSpec(memory_space=pltpu.SMEM)), (own, spec), (cc, spec)] + [(v, piece) for v in list(xx) + list(yy)]
    if final is None:
        return run(kernel, rows // blk, ins, [(jax.ShapeDtypeStruct((rows, cols), F32), spec), (jax.ShapeDtypeStruct((rows, cols), BF), spec)],
                   nbytes=18 * rows * cols, flops=8 * rows * cols)
    arr, shape, layer, rb, cb = final
    aliases = None
    if arr is not None:
        aliases = {len(ins): 0}
        ins.append((arr, ANY))
    fv = (None, (0, 0, layer), (rows, cols), rb, cb)
    return run(kernel, rows // blk, ins, [(jax.ShapeDtypeStruct(shape, F32), by_rows(fv, blk))], aliases, nbytes=14 * rows * cols, flops=8 * rows * cols)


X_SWAP = [(0, 1), (1, 0), (2, 3), (3, 2)]
Y_SWAP = [(0, 2), (2, 0), (1, 3), (3, 1)]
C_SWAP = [(0, 1), (1, 0)]

L1B = ["A", "B", "C"]
ONE0 = ["a0", "a1", "a2", "a3"]
TWO0 = ["b0", "b1", "b2", "b3"]
ONE1 = ["d0", "d1", "d2", "d3"]
N_STEPS = 3
WIRES = [["A"] + ONE1[:2] + ONE0 + TWO0 + ONE1[2:] + ["B", "C"]] * 2 + [["A", "B", "C"] + ONE0 + TWO0 + ONE1]
CUTS = {}
F1_GROUPS = {0: ((0, 1), (2, 3)), 1: ((0, 1), (2,), (3,))}
F1_FIRST = {0: ((0, 1, 2, 3),), 1: ((0, 1, 2, 3),)}
G1_GROUPS = {0: ((0,), (1,), (2, 3)), 1: ((0, 1), (2, 3))}
G2_GROUPS = ((0, 1), (2, 3))
LINK_US = 25.2
START_US = 0.9
MARGIN = 1.5


def pieces(t):
    return [(u, k) for u in WIRES[t] for k in range(CUTS.get(u, 1))]


def f1_groups(t, lay):
    return (F1_GROUPS if t else F1_FIRST)[lay]


def graph():
    ops = {}

    def comp(name, us, needs, pri):
        ops[name] = ("tc", us, list(needs), pri)

    for t in range(N_STEPS):
        def w(units):
            return [f"comb{t - 1}_{u}" for u in units] if t else []

        base = t * 1000
        for lay, names in ((0, ONE0), (1, ONE1)):
            before = [f"f2{t}_0"] if lay else []
            for g, idx in enumerate(f1_groups(t, lay)):
                comp(f"f1{t}_{lay}{g}", {1: 8.8, 2: 13.8, 4: 24.0}[len(idx)] + (0 if t else 2), w([names[j] for j in idx]) + before, base + 10 + 4 * lay + g)
                before = [f"f1{t}_{lay}{g}"]
            if lay == 0:
                comp(f"f2{t}_0", 15, w(TWO0) + before, base + 13)
        for k, u in enumerate(L1B):
            comp(f"fl{t}_{u}", 8.8, w([u]) + before, base + FL_PRI[u])
            comp(f"g2{t}_{u}", 11, [f"fl{t}_{u}"] + w([u]), base + G2_PRI[t][u])
        comp(f"u{t}_1", 19.5, [f"fl{t}_{u}" for u in L1B] + w(L1B), base + 40)
        comp(f"m{t}_0", 17.5, [f"u{t}_1"] + w(ONE1), base + M_PRI)
        for h in (0, 1):
            comp(f"u{t}_0{h}", 11, [f"m{t}_0"] + w(TWO0[2 * h:2 * h + 2]), base + 42 + 10 * h)
        made = {u: f"g2{t}_{u}" for u in L1B}
        for g, idx in enumerate(G1_GROUPS[0]):
            comp(f"g1{t}_0{g}", 14.2 if len(idx) > 1 else 9.5, [f"u{t}_0{j // 2}" for j in idx] + w([ONE0[j] for j in idx]), base + (51, 51.5, 53)[g])
            made.update({ONE0[j]: f"g1{t}_0{g}" for j in idx})
        for g, idx in enumerate(G2_GROUPS):
            comp(f"g2{t}_0{g}", 14.2, [f"m{t}_0"] + w([TWO0[j] for j in idx]), base + 60 + g)
            made.update({TWO0[j]: f"g2{t}_0{g}" for j in idx})
        for g, idx in enumerate(G1_GROUPS[1]):
            comp(f"g1{t}_1{g}", 14.2, [f"u{t}_1"] + w([ONE1[j] for j in idx]), base + G11_PRI[g])
            made.update({ONE1[j]: f"g1{t}_1{g}" for j in idx})
        k = 0
        for u in WIRES[t]:
            n = CUTS.get(u, 1)
            us = LINK_US * (4.0 / 3.0 if u in L1B else 1.0) / n
            for i in range(n):
                ops[f"x{t}_{u}_{i}"] = ("x", us, [made[u]], k)
                ops[f"y{t}_{u}_{i}"] = ("y", us, [f"x{t}_{u}_{i}"], k)
                k += 1
            ops[f"c{t}_{u}"] = ("c", 3, [made[u]], k)
            comp(f"comb{t}_{u}", 6 if u in L1B else 5.5, [f"{r}{t}_{u}_{i}" for r in "xy" for i in range(n)] + [f"c{t}_{u}", made[u]], base + COMB_PRI)
    return ops


FL_PRI = {"A": 20, "B": 22, "C": 24}
G2_PRI = [{"A": 21, "B": 400, "C": 500}] * 2 + [{"A": 21, "B": 23, "C": 25}]
G11_PRI = (40.5, 71)
M_PRI = 41
COMB_PRI = 5


def is_link(name):
    return name[0] in "xyc" and not name.startswith("comb")


def plan():
    ops = graph()
    queue = {r: [f"{r}{t}_{u}_{k}" for t in range(N_STEPS) for u, k in pieces(t)] for r in "xy"}
    queue["c"] = [f"c{t}_{u}" for t in range(N_STEPS) for u in WIRES[t]]
    end = {}
    free = dict.fromkeys("xyc", 0.0)
    order = []
    todo = [n for n in ops if ops[n][0] == "tc"]
    now = 0.0

    def ready_at(n):
        return max([end[d] + (MARGIN if is_link(d) else 0.0) if d in end else 1e9 for d in ops[n][2]], default=0.0)

    while todo or any(queue.values()):
        moved = True
        while moved:
            moved = False
            for r in "yxc":
                while queue[r] and ready_at(queue[r][0]) <= now + 1e-6:
                    n = queue[r].pop(0)
                    now += START_US
                    free[r] = max(now, free[r]) + ops[n][1]
                    end[n] = free[r] + 1.0
                    order.append(n)
                    moved = True
        ready = [n for n in todo if ready_at(n) <= now + 1e-6]
        if ready:
            n = min(ready, key=lambda m: ops[m][3])
            todo.remove(n)
            now += ops[n][1]
            end[n] = now
            order.append(n)
        elif todo or any(queue.values()):
            now = min(x for x in [ready_at(n) for n in todo] + [ready_at(q[0]) for q in queue.values() if q] if x > now)
    return order, max(end.values()), end


def solution(mesh):
    def device_fn(w_one, w_two, inputs, targets):
        _, d, f = w_one.shape[2:]
        rows = inputs.shape[3]
        quarter, third = f // 4, d // 3
        even = (1 - lax.rem(lax.axis_index("row"), 2)).astype(jnp.int32).reshape((1,))
        names = {0: ONE0, 1: ONE1}
        master, where = {}, {}
        for j in range(4):
            for lay in (0, 1):
                where[names[lay][j]] = ("one", lay, (d, quarter), 0, j)
            where[TWO0[j]] = ("two", 0, (quarter, d), j, 0)
        for j, u in enumerate(L1B):
            where[u] = ("two", 1, (f, third), 0, j)
        src = {"one": w_one, "two": w_two}
        for u, (which, lay, shape, rb, cb) in where.items():
            master[u] = view(src[which], (0, 0, lay), shape, rb, cb)
        low = dict(master)
        final = {"one": None, "two": None}
        st, own, wire, cut, moved = {}, {}, {}, {}, {}

        def keep(t, units, got):
            for u, (q, b, parts) in zip(units, got):
                own[t, u], wire[t, u], cut[t, u] = q, b, parts

        def issue(name):
            part = name.split("_")
            t, kind, rest = int(part[0][-1]), part[0][:-1], part[1]
            x_in = view(inputs, (0, 0, t), (rows, d))
            hidden = lambda lay: x_in if lay == 0 else view(st["h", t], (), (rows, d))
            if kind == "x":
                moved[name] = lax.ppermute(cut[t, rest][int(part[2])], "row", X_SWAP)
            elif kind == "y":
                moved[name] = lax.ppermute(moved["x" + name[1:]], "row", Y_SWAP)
            elif kind == "c":
                moved[name] = lax.ppermute(wire[t, rest], "col", C_SWAP)
            elif kind == "comb":
                n = CUTS.get(rest, 1)
                xx, yy = [[moved[f"{r}{t}_{rest}_{k}"] for k in range(n)] for r in "xy"]
                args = (even, own[t, rest], moved[f"c{t}_{rest}"], xx, yy)
                if t == N_STEPS - 1:
                    which, lay, _, rb, cb = where[rest]
                    final[which] = combine(*args, (final[which], src[which].shape, lay, rb, cb))[0]
                else:
                    p, b = combine(*args, None)
                    master[rest], low[rest] = view(p, (), p.shape), view(b, (), b.shape)
            elif kind == "f1":
                lay, g = int(rest[0]), int(rest[1])
                idx = f1_groups(t, lay)[g]
                prev = (st["a", t, lay], st["s", t, lay]) if g else None
                st["a", t, lay], st["s", t, lay] = fwd_one(hidden(lay), [low[names[lay][j]] for j in idx], prev, idx[0])
            elif kind == "f2":
                st["h", t] = fwd_two(x_in, st["a", t, 0], [low[u] for u in TWO0])
            elif kind == "fl":
                target = view(targets, (0, 0, t), (rows, d))
                st["e", t, rest], st["eb", t, rest] = fwd_loss(st["h", t], st["a", t, 1], low[rest], target, L1B.index(rest), d)
            elif kind == "u" and rest == "1":
                st["dz", t, 1] = back_act([st["eb", t, u] for u in L1B], [low[u] for u in L1B], st["s", t, 1])
            elif kind == "u":
                g = int(rest[1])
                st["dz", t, 0, g] = back_act([st["e0", t]], [low[u] for u in TWO0[2 * g:2 * g + 2]], st["s", t, 0], g, 2)
            elif kind == "m":
                st["e0", t] = back_norm(st["dz", t, 1], [low[u] for u in ONE1], hidden(1), [st["e", t, u] for u in L1B])
            elif kind == "g2" and rest in L1B:
                eb, a = st["eb", t, rest], st["a", t, 1]
                keep(t, [rest], grad_update(view(eb, (), eb.shape), view(a, (), a.shape), [master[rest]], [CUTS.get(rest, 1)], False, True))
            else:
                lay, g = int(rest[0]), int(rest[1])
                idx = G1_GROUPS[lay][g] if kind == "g1" else G2_GROUPS[g]
                us = [(names[lay] if kind == "g1" else TWO0)[j] for j in idx]
                n = len(idx)
                if kind == "g2":
                    small, big = view(st["e0", t], (), (rows, d)), view(st["a", t, 0], (), (rows, n * quarter), 0, idx[0] // n)
                elif lay == 1:
                    small, big = hidden(1), view(st["dz", t, 1], (), (rows, n * quarter), 0, idx[0] // n)
                else:
                    small, big = x_in, view(st["dz", t, 0, idx[0] // 2], (), (rows, n * quarter), 0, (idx[0] % 2) // n)
                keep(t, us, grad_update(small, big, [master[u] for u in us], [CUTS.get(u, 1) for u in us], kind == "g1", kind == "g2"))

        for name in plan()[0]:
            issue(name)
        return final["one"], final["two"]

    spec = P("row", "col")
    return jax.shard_map(device_fn, mesh=mesh, in_specs=(spec,) * 4, out_specs=(spec, spec), check_vma=False)
```

```python
import jax
import jax.numpy as jnp
from jax import lax
from jax.experimental import pallas as pl
from jax.experimental.pallas import tpu as pltpu
from jax.sharding import PartitionSpec as P


LEARN_RATE = 1.5
NORM_EPS = 1e-6
GELU_C = 0.7978845608028654
GELU_K = 0.044715

BF = jnp.bfloat16
F32 = jnp.float32
VMEM_LIMIT = 60 * 1024 * 1024
ROWS = 256
MROWS = 512
LROWS = 1024
BROWS = 256
CROWS = 512
KROWS = 512
SUB = 256


ANY = pl.BlockSpec(memory_space=pl.ANY)


def nn(lhs, rhs):
    return lax.dot_general(lhs, rhs, (((1,), (0,)), ((), ())), preferred_element_type=F32)


def nt(lhs, rhs):
    return lax.dot_general(lhs, rhs, (((1,), (1,)), ((), ())), preferred_element_type=F32)


def gelu_slope(z):
    z2 = z * z
    t = jnp.tanh(z * (GELU_C + (GELU_C * GELU_K) * z2))
    half = 0.5 + 0.5 * t
    return half + z * half * (1.0 - t) * (GELU_C + (3.0 * GELU_C * GELU_K) * z2)


def view(arr, lead, shape, row_blk=0, col_blk=0):
    return (arr, lead, shape, row_blk, col_blk)


def whole(v):
    _, lead, shape, rb, cb = v
    return pl.BlockSpec((None,) * len(lead) + shape, lambda i: lead + (rb, cb))


def by_rows(v, rows):
    _, lead, shape, rb, cb = v
    steps = shape[0] // rows
    return pl.BlockSpec((None,) * len(lead) + (rows, shape[1]), lambda i: lead + (rb * steps + i, cb))


def run(kernel, grid, ins, outs, aliases=None, scratch=(), flops=0, nbytes=0):
    return pl.pallas_call(
        kernel,
        grid=(grid,),
        in_specs=[spec for _, spec in ins],
        out_specs=[spec for _, spec in outs],
        out_shape=[shape for shape, _ in outs],
        input_output_aliases=aliases or {},
        scratch_shapes=list(scratch),
        compiler_params=pltpu.CompilerParams(dimension_semantics=("arbitrary",), vmem_limit_bytes=VMEM_LIMIT),
        cost_estimate=pl.CostEstimate(flops=int(flops), bytes_accessed=int(nbytes), transcendentals=0),
    )(*[v[0] if isinstance(v, tuple) else v for v, _ in ins])


def norm_of(h):
    x = h.astype(F32)
    inv = lax.rsqrt(jnp.mean(x * x, axis=-1, keepdims=True) + NORM_EPS)
    return x * inv, inv


def fwd_one(h, units, prev, off, keep_z):
    rows, d = h[2]
    width = units[0][2][1]
    f = 4 * width
    nu = len(units)
    cast = int(units[0][0].dtype == F32)
    rb = ROWS if nu > 1 else 2 * ROWS

    def kernel(h_ref, *refs):
        w_refs, (a_ref, s_ref) = refs[:nu], refs[-2 - cast:len(refs) - cast]
        if cast:
            low_ref = refs[-1]

            @pl.when(pl.program_id(0) == 0)
            def _():
                for j in range(nu):
                    low_ref[j] = w_refs[j][...].astype(BF)

            w_refs = [low_ref.at[j] for j in range(nu)]
        n, _ = norm_of(h_ref[...])
        n = n.astype(BF)
        for j in range(nu):
            for c in range(0, width, SUB):
                z = nn(n, w_refs[j][:, c:c + SUB])
                z2 = z * z
                t = jnp.tanh(z * (GELU_C + (GELU_C * GELU_K) * z2))
                cols = slice(j * width + c, j * width + c + SUB)
                half = 0.5 + 0.5 * t
                a_ref[:, cols] = (z * half).astype(BF)
                s_ref[:, cols] = z if keep_z else half + z * half * (1.0 - t) * (GELU_C + (3.0 * GELU_C * GELU_K) * z2)

    blk = pl.BlockSpec((rb, nu * width), lambda i: (i, off // nu))
    ins = [(h, by_rows(h, rb))] + [(u, whole(u)) for u in units]
    aliases = None
    if prev is not None:
        aliases = {len(ins): 0, len(ins) + 1: 1}
        ins += [(p, ANY) for p in prev]
    return run(kernel, rows // rb, ins, [(jax.ShapeDtypeStruct((rows, f), BF), blk), (jax.ShapeDtypeStruct((rows, f), F32), blk)],
               aliases, scratch=[pltpu.VMEM((nu, d, width), BF)] * cast, flops=2 * rows * d * width * nu, nbytes=6 * rows * width * nu)


def fwd_two(h, a, units):
    rows, d = h[2]
    nu = len(units)
    f = a.shape[1]
    part = f // nu
    av = view(a, (), (rows, f))

    def kernel(h_ref, a_ref, *refs):
        w_refs, o_ref = refs[:nu], refs[nu]
        for c in range(0, d, SUB):
            acc = nn(a_ref[:, :part], w_refs[0][:, c:c + SUB].astype(BF))
            for j in range(1, nu):
                acc += nn(a_ref[:, j * part:(j + 1) * part], w_refs[j][:, c:c + SUB].astype(BF))
            o_ref[:, c:c + SUB] = (h_ref[:, c:c + SUB].astype(F32) + acc).astype(BF)

    ov = view(None, (), (rows, d))
    return run(kernel, rows // MROWS, [(h, by_rows(h, MROWS)), (av, by_rows(av, MROWS))] + [(u, whole(u)) for u in units],
               [(jax.ShapeDtypeStruct((rows, d), BF), by_rows(ov, MROWS))], flops=2 * rows * d * f, nbytes=2 * rows * f)[0]


def fwd_loss(h, a, units, target, idxs, d):
    rows, f = a.shape
    nu = len(units)
    rb = LROWS if nu == 1 else LROWS // 2
    w = units[0][2][1]
    scale = 2.0 / (rows * d)
    hs = [view(h, (), (rows, w), 0, i) for i in idxs]
    ts = [view(target[0], target[1], (rows, w), 0, i) for i in idxs]
    av = view(a, (), (rows, f))

    def kernel(a_ref, *refs):
        h_refs, t_refs, w_refs, o_refs = refs[:nu], refs[nu:2 * nu], refs[2 * nu:3 * nu], refs[3 * nu:]
        for j in range(nu):
            out = (h_refs[j][...].astype(F32) + nn(a_ref[...], w_refs[j][...].astype(BF))).astype(BF)
            e = scale * (out.astype(F32) - t_refs[j][...].astype(F32))
            o_refs[j][...] = e
            o_refs[nu + j][...] = e.astype(BF)

    ov = view(None, (), (rows, w))
    res = run(kernel, rows // rb, [(av, by_rows(av, rb))] + [(v, by_rows(v, rb)) for v in hs + ts] + [(u, whole(u)) for u in units],
              [(jax.ShapeDtypeStruct((rows, w), dt), by_rows(ov, rb)) for dt in (F32, BF) for _ in units],
              flops=2 * rows * w * nu * f, nbytes=2 * rows * f)
    return res[:nu], res[nu:]


def back_both(errs, twos, slope, ones, h, wide, from_z):
    rows, f = slope.shape
    d = h[2][1]
    ne, nu = len(errs), len(ones)
    per, w = f // nu, d // ne

    def kernel(s_ref, h_ref, *refs):
        e_refs, w2_refs, w1_refs, x_refs = refs[:ne], refs[ne:2 * ne], refs[2 * ne:2 * ne + nu], refs[2 * ne + nu:3 * ne + nu]
        dz_ref, o_ref, m_ref = refs[-3:]
        for c in range(0, f, SUB):
            u = nt(e_refs[0][...], w2_refs[0][c:c + SUB, :].astype(BF))
            for k in range(1, ne):
                u += nt(e_refs[k][...], w2_refs[k][c:c + SUB, :].astype(BF))
            dz_ref[:, c:c + SUB] = (u * (gelu_slope(s_ref[:, c:c + SUB]) if from_z else s_ref[:, c:c + SUB])).astype(BF)
        for c in range(0, d, SUB):
            m = nt(dz_ref[:, :per], w1_refs[0][c:c + SUB, :].astype(BF))
            for j in range(1, nu):
                m += nt(dz_ref[:, j * per:(j + 1) * per], w1_refs[j][c:c + SUB, :].astype(BF))
            m_ref[:, c:c + SUB] = m
        n, inv = norm_of(h_ref[...])
        m = m_ref[...]
        back = inv * (m - n * jnp.mean(m * n, axis=-1, keepdims=True))
        for k in range(ne):
            o_ref[:, k * w:(k + 1) * w] = (x_refs[k][...] + back[:, k * w:(k + 1) * w]).astype(BF)

    sv = view(slope, (), (rows, f))
    ov = view(None, (), (rows, d))
    rb = BROWS
    return run(kernel, rows // rb,
               [(sv, by_rows(sv, rb)), (h, by_rows(h, rb))] + [(view(e, (), e.shape), by_rows(view(e, (), e.shape), rb)) for e in errs]
               + [(u, whole(u)) for u in list(twos) + list(ones)] + [(view(e, (), e.shape), by_rows(view(e, (), e.shape), rb)) for e in wide],
               [(jax.ShapeDtypeStruct((rows, f), BF), by_rows(sv, rb)), (jax.ShapeDtypeStruct((rows, d), BF), by_rows(ov, rb))],
               scratch=[pltpu.VMEM((rb, d), F32)], flops=4 * rows * f * d, nbytes=10 * rows * f)


def grad_cols(errs, a, olds, cuts):
    rows, w = errs[0].shape
    f = a.shape[1]
    nu = len(olds)
    kr = CROWS
    steps = rows // kr
    outs, kinds = [], []
    for j in range(nu):
        outs += [jax.ShapeDtypeStruct((f, w), F32), jax.ShapeDtypeStruct((f, w), BF)] + [jax.ShapeDtypeStruct((f // cuts[j], w), BF)] * (cuts[j] if cuts[j] > 1 else 0)
        kinds += [(j, -2), (j, -1)] + [(j, k) for k in range(cuts[j] if cuts[j] > 1 else 0)]

    def kernel(a_ref, *refs):
        e_refs, p_refs, o_refs, acc_ref = refs[:nu], refs[nu:2 * nu], dict(zip(kinds, refs[2 * nu:-1])), refs[-1]
        i = pl.program_id(0)
        sts = [e_ref[...].T for e_ref in e_refs]

        @pl.when(i == 0)
        def _():
            for j in range(nu):
                for c in range(0, f, SUB):
                    acc_ref[j * w:(j + 1) * w, c:c + SUB] = nn(sts[j], a_ref[:, c:c + SUB])

        @pl.when(i > 0)
        def _():
            for j in range(nu):
                for c in range(0, f, SUB):
                    acc_ref[j * w:(j + 1) * w, c:c + SUB] += nn(sts[j], a_ref[:, c:c + SUB])

        @pl.when(i == steps - 1)
        def _():
            for j in range(nu):
                size = f // cuts[j]
                for c in range(0, f, SUB):
                    q = p_refs[j][c:c + SUB, :] - LEARN_RATE * acc_ref[j * w:(j + 1) * w, c:c + SUB].T
                    low = q.astype(BF)
                    o_refs[j, -2][c:c + SUB, :] = q
                    o_refs[j, -1][c:c + SUB, :] = low
                    if cuts[j] > 1:
                        o_refs[j, c // size][c % size:c % size + SUB, :] = low

    av = view(a, (), (rows, f))
    es = [view(e, (), (rows, w)) for e in errs]
    res = run(kernel, steps, [(av, by_rows(av, kr))] + [(e, by_rows(e, kr)) for e in es] + [(u, whole(u)) for u in olds],
              [(o, pl.BlockSpec(o.shape, lambda i: (0, 0))) for o in outs], scratch=[pltpu.VMEM((nu * w, f), F32)],
              flops=2 * rows * nu * w * f, nbytes=2 * rows * f)
    got = dict(zip(kinds, res))
    return [(got[j, -2], got[j, -1], [got[j, k] for k in range(cuts[j])] if cuts[j] > 1 else [got[j, -1]]) for j in range(nu)]


def back_act(errs, units, slope, from_z, lo=0, of=1):
    rows, f = slope.shape
    f = f // of
    ne, nu = len(errs), len(units)
    rb = MROWS // 2 if from_z and of == 1 else MROWS
    per = units[0][2][0]

    def kernel(*refs):
        e_refs, w_refs = refs[:ne], refs[ne:ne + nu]
        s_ref, o_ref = refs[ne + nu:]
        for c in range(0, f, SUB):
            if ne > 1:
                u = nt(e_refs[0][...], w_refs[0][c:c + SUB, :].astype(BF))
                for k in range(1, ne):
                    u += nt(e_refs[k][...], w_refs[k][c:c + SUB, :].astype(BF))
            else:
                r = c % per
                u = nt(e_refs[0][...], w_refs[c // per][r:r + SUB, :].astype(BF))
            o_ref[:, c:c + SUB] = (u * (gelu_slope(s_ref[:, c:c + SUB]) if from_z else s_ref[:, c:c + SUB])).astype(BF)

    if ne > 1:
        units = [view(arr, lead, (f, shape[1]), lo, cb) for arr, lead, shape, _, cb in units]
    vs = [view(e, (), e.shape) for e in errs]
    sv = view(slope, (), (rows, f), 0, lo)
    ov = view(None, (), (rows, f))
    return run(kernel, rows // rb, [(v, by_rows(v, rb)) for v in vs] + [(u, whole(u)) for u in units] + [(sv, by_rows(sv, rb))],
               [(jax.ShapeDtypeStruct((rows, f), BF), by_rows(ov, rb))], flops=2 * rows * f * 768, nbytes=6 * rows * f)[0]


def back_norm(dzs, units, h, errs):
    rows, fp = dzs[0].shape
    nd = len(dzs)
    f = fp * nd
    d = h[2][1]
    ne, nu = len(errs), len(units)
    per = f // nu

    def kernel(*refs):
        dz_refs, refs = refs[:nd], refs[nd:]
        part = lambda j: dz_refs[j * per // fp][:, j * per % fp:j * per % fp + per]
        w_refs, h_ref, e_refs, o_ref, m_ref = refs[:nu], refs[nu], refs[nu + 1:nu + 1 + ne], refs[-2], refs[-1]
        for c in range(0, d, SUB):
            m = nt(part(0), w_refs[0][c:c + SUB, :].astype(BF))
            for j in range(1, nu):
                m += nt(part(j), w_refs[j][c:c + SUB, :].astype(BF))
            m_ref[:, c:c + SUB] = m
        n, inv = norm_of(h_ref[...])
        m = m_ref[...]
        back = inv * (m - n * jnp.mean(m * n, axis=-1, keepdims=True))
        w = d // ne
        for k in range(ne):
            o_ref[:, k * w:(k + 1) * w] = (e_refs[k][...] + back[:, k * w:(k + 1) * w]).astype(BF)

    dv = view(None, (), (rows, fp))
    vs = [view(e, (), e.shape) for e in errs]
    ov = view(None, (), (rows, d))
    return run(kernel, rows // MROWS,
               [(dz, by_rows(dv, MROWS)) for dz in dzs] + [(u, whole(u)) for u in units] + [(h, by_rows(h, MROWS))] + [(v, by_rows(v, MROWS)) for v in vs],
               [(jax.ShapeDtypeStruct((rows, d), BF), by_rows(ov, MROWS))], scratch=[pltpu.VMEM((MROWS, d), F32)],
               flops=2 * rows * f * d, nbytes=2 * rows * f)[0]


def grad_update(small, big, olds, cuts, use_norm, flip):
    rows, m = small[2]
    n = big[2][1]
    nu = len(olds)
    per = n // nu
    steps = rows // KROWS
    out_shapes, out_kinds = [], []
    for j, u in enumerate(olds):
        r, c = u[2]
        out_shapes += [((r, c), F32), ((r, c), BF)] + ([((r // cuts[j], c), BF)] * cuts[j] if cuts[j] > 1 else [])
        out_kinds += [(j, -2), (j, -1)] + ([(j, k) for k in range(cuts[j])] if cuts[j] > 1 else [])

    def kernel(s_ref, b_ref, *refs):
        p_refs, o_refs, acc_ref = refs[:nu], refs[nu:-1], refs[-1]
        i = pl.program_id(0)
        s = s_ref[...]
        if use_norm:
            s = norm_of(s)[0].astype(BF)
        st = s.T

        @pl.when(i == 0)
        def _():
            for c in range(0, n, SUB):
                acc_ref[:, c:c + SUB] = nn(st, b_ref[:, c:c + SUB])

        @pl.when(i > 0)
        def _():
            for c in range(0, n, SUB):
                acc_ref[:, c:c + SUB] += nn(st, b_ref[:, c:c + SUB])

        @pl.when(i == steps - 1)
        def _():
            for (j, kind), o_ref in zip(out_kinds, o_refs):
                if kind != -2:
                    continue
                w_ref = o_refs[out_kinds.index((j, -1))]
                pieces = [o_refs[out_kinds.index((j, k))] for k in range(cuts[j])] if cuts[j] > 1 else []
                size = olds[j][2][0] // cuts[j]
                for c in range(0, per, SUB):
                    g = acc_ref[:, j * per + c:j * per + c + SUB]
                    at = (slice(c, c + SUB), slice(None)) if flip else (slice(None), slice(c, c + SUB))
                    q = p_refs[j][at] - LEARN_RATE * (g.T if flip else g)
                    low = q.astype(BF)
                    o_ref[at] = q
                    w_ref[at] = low
                    for k, piece in enumerate(pieces):
                        if flip:
                            lo, hi = max(c, k * size), min(c + SUB, (k + 1) * size)
                            if lo < hi:
                                piece[lo - k * size:hi - k * size, :] = low[lo - c:hi - c]
                        else:
                            piece[:, c:c + SUB] = low[k * size:(k + 1) * size]

    res = run(kernel, steps, [(small, by_rows(small, KROWS)), (big, by_rows(big, KROWS))] + [(u, whole(u)) for u in olds],
              [(jax.ShapeDtypeStruct(sh, dt), pl.BlockSpec(sh, lambda i: (0, 0))) for sh, dt in out_shapes],
              scratch=[pltpu.VMEM((m, n), F32)], flops=2 * rows * m * n, nbytes=10 * m * n)
    got = {kind: r for kind, r in zip(out_kinds, res)}
    return [(got[j, -2], got[j, -1], [got[j, k] for k in range(cuts[j])] if cuts[j] > 1 else [got[j, -1]]) for j in range(nu)]


COMB_ROWS = {768: 384, 256: 1536}


def combine(even, own, cc, xx, yy, final):
    rows, cols = own.shape
    nc = len(xx)
    blk = rows // nc if nc > 1 else COMB_ROWS[cols]

    def kernel(even_ref, q_ref, c_ref, *refs):
        def mix(x, y):
            prev = jnp.where(even_ref[0] == 1, y, x).astype(F32)
            nxt = jnp.where(even_ref[0] == 1, x, y).astype(F32)
            c = c_ref[...].astype(F32)
            p = (q_ref[...] + c + c + prev + nxt) / 5.0
            if final is None:
                refs[2 * nc][...] = p
                refs[2 * nc + 1][...] = p.astype(BF)
            else:
                refs[-1][...] = p

        if nc == 1:
            mix(refs[0][...], refs[1][...])
        else:
            for k in range(nc):
                @pl.when(pl.program_id(0) == k)
                def _(k=k):
                    mix(refs[k][...], refs[nc + k][...])

    ov = view(None, (), (rows, cols))
    spec = by_rows(ov, blk)
    pv = view(None, (), (rows // nc, cols))
    piece = by_rows(pv, blk) if nc == 1 else whole(pv)
    ins = [(even, pl.BlockSpec(memory_space=pltpu.SMEM)), (own, spec), (cc, spec)] + [(v, piece) for v in list(xx) + list(yy)]
    if final is None:
        return run(kernel, rows // blk, ins, [(jax.ShapeDtypeStruct((rows, cols), F32), spec), (jax.ShapeDtypeStruct((rows, cols), BF), spec)],
                   nbytes=18 * rows * cols, flops=8 * rows * cols)
    arr, shape, layer, rb, cb = final
    aliases = None
    if arr is not None:
        aliases = {len(ins): 0}
        ins.append((arr, ANY))
    fv = (None, (0, 0, layer), (rows, cols), rb, cb)
    return run(kernel, rows // blk, ins, [(jax.ShapeDtypeStruct(shape, F32), by_rows(fv, blk))], aliases, nbytes=14 * rows * cols, flops=8 * rows * cols)


X_SWAP, Y_SWAP = [[(r, r ^ bit) for r in range(4)] for bit in (1, 2)]
C_SWAP = [(c, 1 - c) for c in range(2)]

L1B = ["A", "B", "C"]
ONE0, TWO0, ONE1 = [[f"{k}{j}" for j in range(4)] for k in "abd"]
UNITS = L1B + ONE0 + TWO0 + ONE1
KINDS = "comb f1 f2 fl".split() + "gl g1 g2 u".split() + ["m", "v"]
PLAN = [
    {
        "wires": (11121006090403, 7080513140102), "halved": 25278,
        "f1": ((4,), (4,)), "g1": ((2, 2), (2, 2)), "g2": (1, 1, 1, 1),
        "fl": (123,), "gl": (1, 23), "u0": 1, "u1": 1, "z": (1, 1),
    },
    {
        "wires": (12110708040305, 10060913140201), "halved": 12782,
        "f1": ((2, 2), (2, 2)), "g1": ((2, 1, 1), (2, 2)), "g2": (2, 2),
        "fl": (1, 2, 3), "gl": (1, 23), "u0": 1, "u1": 2, "z": (0, 0),
    },
    {
        "wires": (2011411081007, 5130406030912), "halved": 26716,
        "f1": ((2, 1, 1), (2, 1, 1)), "g1": ((2, 2), (1, 1, 1, 1)), "g2": (2, 1, 1),
        "fl": (1, 2, 3), "gl": (1, 2, 3), "u0": 2, "u1": 1, "z": (0, 0),
    },
]

LAST = 3
CALLS = [
    100000002000000010100000, 300000004000000070100011, 501000008000102260030000, 700010115001100000110011,
    600210005000002150111042, 600010000010102140011000, 600120000000211600031000, 600000009000000071000,
    1210000004000011000000, 820000005100011011000, 210010001110100000141000, 1300001111000031001000,
    410010000001001131010000, 200003102000071100000, 511010007111003281001000, 610010007100104201001000,
    510010005111103201121000, 11100005101100051021021, 610100000108307541010000, 10410420107100001030000,
    120010000110000001050000, 120110000106000012021000, 10910002200000012101000, 11300001211100001140000,
    121210003200000042001000, 10210113202000042020000, 10100213201100042010000, 920010115213100052101021,
    720010216200100052121011, 720110006202000062011022, 20100005201000002021032, 520000005211107402111011,
    21400000200100002080000, 20510000207100002043000, 21310000210000002061000, 20920000203000002120000,
]
N_STEPS = len(PLAN)


def spans(sizes):
    return [tuple(range(sum(sizes[:k]), sum(sizes[:k + 1]))) for k in range(len(sizes))]


for _cfg in PLAN:
    _digits = "".join(str(n).zfill(size) for n, size in zip(_cfg["wires"], (16, 14)))
    _cfg["wires"] = [UNITS[int(_digits[i:i + 2])] for i in range(0, len(_digits), 2)]
    _cfg["halved"] = [u for i, u in enumerate(UNITS) if _cfg["halved"] >> i & 1]
    for _key in ("fl", "gl"):
        _cfg[_key] = [[L1B[int(i) - 1] for i in str(group)] for group in _cfg[_key]]
    _cfg["f1"], _cfg["g1"] = [[spans(v) for v in _cfg[_key]] for _key in ("f1", "g1")]
    _cfg["g2"] = spans(_cfg["g2"])


def halves(t, u):
    return 2 if u in PLAN[t]["halved"] else 1


def issue_order():
    units = [(t, u) for t in range(N_STEPS) for u in PLAN[t]["wires"]]
    both = [f"{t}_{u}_{k}" for t, u in units for k in range(halves(t, u))]
    queue = {"y": iter(both), "x": iter(both), "c": iter([f"{t}_{u}" for t, u in units])}
    order = []
    digits = "".join(str(n).zfill(24) for n in CALLS[:-1]) + str(CALLS[-1]).zfill(8 * LAST)
    for i in range(0, len(digits), 8):
        code = digits[i:i + 8]
        kind, t, arg = KINDS[int(code[0])], code[1], code[2:4]
        for link, count in (("y", code[4]), ("x", code[5:7]), ("c", code[7])):
            order += [link + next(queue[link]) for _ in range(int(count))]
        if kind == "comb":
            arg = UNITS[int(arg)]
        elif kind not in ("f1", "g1", "g2", "u"):
            arg = str(int(arg))
        order.append(f"{kind}{t}_{arg}")
    return order


ORDER = issue_order()


def solution(mesh):
    def device_fn(w_one, w_two, inputs, targets):
        _, d, f = w_one.shape[2:]
        rows = inputs.shape[3]
        quarter, third = f // 4, d // 3
        even = (1 - lax.rem(lax.axis_index("row"), 2)).astype(jnp.int32).reshape((1,))
        names = {0: ONE0, 1: ONE1}
        master, where = {}, {}
        for j in range(4):
            for lay in (0, 1):
                where[names[lay][j]] = ("one", lay, (d, quarter), 0, j)
            where[TWO0[j]] = ("two", 0, (quarter, d), j, 0)
        for j, u in enumerate(L1B):
            where[u] = ("two", 1, (f, third), 0, j)
        src = {"one": w_one, "two": w_two}
        for u, (which, lay, shape, rb, cb) in where.items():
            master[u] = view(src[which], (0, 0, lay), shape, rb, cb)
        low = dict(master)
        final = {"one": None, "two": None}
        st, own, wire, cut, moved = {}, {}, {}, {}, {}

        def keep(t, units, got):
            for u, (q, b, parts) in zip(units, got):
                own[t, u], wire[t, u], cut[t, u] = q, b, parts

        def issue(name):
            part = name.split("_")
            t, kind, rest = int(part[0][-1]), part[0][:-1], part[1]
            cfg = PLAN[t]
            x_in = view(inputs, (0, 0, t), (rows, d))
            hidden = lambda lay: x_in if lay == 0 else view(st["h", t], (), (rows, d))
            lows = lambda us: [low[u] for u in us]
            if kind == "x":
                moved[name] = lax.ppermute(cut[t, rest][int(part[2])], "row", X_SWAP)
            elif kind == "y":
                moved[name] = lax.ppermute(moved["x" + name[1:]], "row", Y_SWAP)
            elif kind == "c":
                moved[name] = lax.ppermute(wire[t, rest], "col", C_SWAP)
            elif kind == "comb":
                xx, yy = [[moved[f"{r}{t}_{rest}_{k}"] for k in range(halves(t, rest))] for r in "xy"]
                args = (even, own[t, rest], moved[f"c{t}_{rest}"], xx, yy)
                if t == N_STEPS - 1:
                    which, lay, _, rb, cb = where[rest]
                    final[which] = combine(*args, (final[which], src[which].shape, lay, rb, cb))[0]
                else:
                    p, b = combine(*args, None)
                    master[rest], low[rest] = view(p, (), p.shape), view(b, (), b.shape)
            elif kind == "f1":
                lay, g = int(rest[0]), int(rest[1])
                idx = cfg["f1"][lay][g]
                prev = (st["a", t, lay], st["s", t, lay]) if g else None
                st["a", t, lay], st["s", t, lay] = fwd_one(hidden(lay), lows(names[lay][j] for j in idx), prev, idx[0], cfg["z"][lay])
            elif kind == "f2":
                st["h", t] = fwd_two(x_in, st["a", t, 0], lows(TWO0))
            elif kind == "fl":
                us = cfg["fl"][int(rest)]
                target = view(targets, (0, 0, t), (rows, d))
                wide, eb = fwd_loss(st["h", t], st["a", t, 1], lows(us), target, [L1B.index(u) for u in us], d)
                for k, u in enumerate(us):
                    st["e", t, u], st["eb", t, u] = wide[k], eb[k]
            elif kind == "v":
                st["dz", t, 1, 0], st["e0", t] = back_both([st["eb", t, u] for u in L1B], lows(L1B), st["s", t, 1], lows(ONE1), hidden(1), [st["e", t, u] for u in L1B], cfg["z"][1])
            elif kind == "u" and rest[0] == "1":
                g, of = int(rest[1]), cfg["u1"]
                st["dz", t, 1, g] = back_act([st["eb", t, u] for u in L1B], lows(L1B), st["s", t, 1], cfg["z"][1], g, of)
            elif kind == "m":
                st["e0", t] = back_norm([st["dz", t, 1, g] for g in range(cfg["u1"])], lows(ONE1), hidden(1), [st["e", t, u] for u in L1B])
            elif kind == "u":
                g, of = int(rest[1]), cfg["u0"]
                st["dz", t, 0, g] = back_act([st["e0", t]], lows(TWO0[4 // of * g:4 // of * (g + 1)]), st["s", t, 0], cfg["z"][0], g, of)
            elif kind == "gl":
                us = cfg["gl"][int(rest)]
                keep(t, us, grad_cols([st["eb", t, u] for u in us], st["a", t, 1], [master[u] for u in us], [halves(t, u) for u in us]))
            else:
                lay, g = int(rest[0]), int(rest[1])
                idx = cfg["g1"][lay][g] if kind == "g1" else cfg["g2"][g]
                us = [(names[lay] if kind == "g1" else TWO0)[j] for j in idx]
                n = len(idx)
                if kind == "g2":
                    small, big = view(st["e0", t], (), (rows, d)), view(st["a", t, 0], (), (rows, n * quarter), 0, idx[0] // n)
                else:
                    per = 4 // cfg["u1" if lay else "u0"]
                    small, big = hidden(lay), view(st["dz", t, lay, idx[0] // per], (), (rows, n * quarter), 0, (idx[0] % per) // n)
                keep(t, us, grad_update(small, big, [master[u] for u in us], [halves(t, u) for u in us], kind == "g1", kind == "g2"))

        for name in ORDER:
            issue(name)
        return final["one"], final["two"]

    spec = P("row", "col")
    return jax.shard_map(device_fn, mesh=mesh, in_specs=(spec,) * 4, out_specs=(spec, spec), check_vma=False)
```
